32 devices in a mesh: mx: 4 (over z), my: 4 (over y, core), col: 2 (over x).
Axes of the slice: x: 2, y: 2, z: 4, core: 2. Of those that a mesh axis runs over, the one named last changes fastest.
Arguments:
- spectrum: float32 [2, 4, 128, 32, 512], P(None, 'col', None, 'mx', 'my'), may hold values from -6 to 6
- core_tensor: float32 [2, 64, 64, 16, 16, 16], P(None, 'col', None, ('mx', 'my')), may hold values from -0.01171875 to 0.01171875
- input_factor: float32 [128, 64], replicated, may hold values from -0.5 to 0.5
- output_factor: float32 [128, 64], replicated, may hold values from -0.75 to 0.75
- first_factor: float32 [32, 16], P('mx'), may hold values from -5 to 5
- second_factor: float32 [32, 16], P('my'), may hold values from -5 to 5
- third_factor: float32 [16, 16], replicated, may hold values from -5 to 5
Outputs:
- mixed_modes: float32 [2, 4, 128, 32, 512], P(None, 'col', None, 'mx', 'my')
The draws below stay inside these ranges and needn't reach their ends.
All inputs are finite; a program needn't handle non-finite values.
Results may differ from the reference program's by a relative error of at most 0.00007.
Values sent between devices are 32-bit elements; how exact they have to be, the bound alone decides.
A program may use at most 192 MiB of HBM per device.

```python
import jax
import jax.numpy as jnp
from jax import lax

CIN = 128
COUT = 128
R1 = 64
R2 = 64
R3 = 16
R4 = 16
R5 = 16
KX = 32
KY = 32
KZ = 16
BATCH = 4


def block_scale(key, extent, split, low, largest):
    level, own = 1.0, jax.random.fold_in(key, 6)
    for dim, blocks in split:
        steps = jnp.exp(jax.random.uniform(jax.random.fold_in(own, dim), (blocks,), jnp.float32, low / len(split), largest / len(split)))
        level = level * jnp.repeat(steps, extent[dim] // blocks).reshape([-1 if axis == dim else 1 for axis in range(len(extent))])
    return level


def bell_draw(own_key, shape, width, most, split=(), held_as=jnp.bfloat16):
    values = width * jax.random.normal(own_key, shape, jnp.float32)
    if split:
        values = values * block_scale(own_key, shape, split, -0.22, 0.18)
    return jnp.clip(values, -most, most).astype(held_as)


def setup_inputs(seed: int = 0) -> dict:
    arg_keys = jax.random.split(jax.random.key(seed), 8)
    spectrum = bell_draw(arg_keys[0], (2, BATCH, CIN, KX, KY * KZ), 1.0, 6.0, ((1, 2), (3, 4), (4, 4)), jnp.float32)
    core_tensor = bell_draw(arg_keys[1], (2, R1, R2, R3, R4, R5), (R1 * R3 * R4 * R5) ** -0.5, 0.01171875, ((1, 2), (3, 16)), jnp.float32)
    input_factor = bell_draw(arg_keys[2], (CIN, R1), CIN ** -0.5, 0.5, (), jnp.float32)
    output_factor = bell_draw(arg_keys[3], (COUT, R2), R2 ** -0.5, 0.75, (), jnp.float32)
    first_factor = bell_draw(arg_keys[4], (KX, R3), 1.0, 5.0, ((0, 4),), jnp.float32)
    second_factor = bell_draw(arg_keys[5], (KY, R4), 1.0, 5.0, ((0, 4),), jnp.float32)
    third_factor = bell_draw(arg_keys[6], (KZ, R5), 1.0, 5.0, (), jnp.float32)
    return {"spectrum": spectrum, "core_tensor": core_tensor, "input_factor": input_factor, "output_factor": output_factor, "first_factor": first_factor, "second_factor": second_factor, "third_factor": third_factor}


def reference(spectrum, core_tensor, input_factor, output_factor, first_factor, second_factor, third_factor):
    precise = lax.Precision.HIGHEST
    rank_spectrum = jnp.einsum('cbikm,ir->cbrkm', spectrum, input_factor, precision=precise)
    core_third = jnp.einsum('cpqstu,zu->cpqstz', core_tensor, third_factor, precision=precise)
    core_second = jnp.einsum('cpqstz,yt->cpqsyz', core_third, second_factor, precision=precise)
    core_second = core_second.reshape(2, R1, R2, R3, KY * KZ)

    def per_mode_row(inputs):
        spectrum_row, factor_row = inputs
        weight_row = jnp.einsum('cpqsm,s->cpqm', core_second, factor_row, precision=precise)
        real_part = jnp.einsum('brm,rqm->bqm', spectrum_row[0], weight_row[0], precision=precise) - jnp.einsum('brm,rqm->bqm', spectrum_row[1], weight_row[1], precision=precise)
        imag_part = jnp.einsum('brm,rqm->bqm', spectrum_row[0], weight_row[1], precision=precise) + jnp.einsum('brm,rqm->bqm', spectrum_row[1], weight_row[0], precision=precise)
        mode_values = jnp.stack([real_part, imag_part])
        return jnp.einsum('oq,cbqm->cbom', output_factor, mode_values, precision=precise)

    mixed_rows = lax.map(per_mode_row, (jnp.moveaxis(rank_spectrum, 3, 0), first_factor))
    return jnp.moveaxis(mixed_rows, 0, 3)
```

```python
import functools

import jax
import jax.numpy as jnp
from jax import lax
from jax.experimental import pallas as pl
from jax.experimental.pallas import tpu as pltpu
from jax.sharding import PartitionSpec as P

MESH = pl.DeviceIdType.MESH
F32 = jnp.float32
BF16 = jnp.bfloat16


def halves(value):
    high = value.astype(BF16)
    return high, (value - high.astype(F32)).astype(BF16)


def dot_split(left, right):
    (lh, ll), (rh, rl) = left, right
    dot = functools.partial(jnp.dot, preferred_element_type=F32)
    return dot(lh, rh) + (dot(lh, rl) + dot(ll, rh))


def kernel(
    dims,
    spec_ref, core_hbm, kin_ref, ktu_ref, kf1_ref, kout_ref,
    out_ref,
    core_v, xs, X, E, G, Y, R, W, ktu_s, kf1_s,
    core_sem, xsend, xrecv, esend, erecv, ysend, yrecv,
):
    nx, ny, nc, chunks, pc, group = dims
    n_s = nx * ny
    mx, my, col = lax.axis_index("mx"), lax.axis_index("my"), lax.axis_index("col")
    b_loc, cin, kx_loc, lanes = spec_ref.shape[1:]
    p_loc = X.shape[4]
    q_loc = G.shape[4]
    q_all = core_hbm.shape[3]
    cout = out_ref.shape[2]
    me_s = mx * ny + my
    me_c = mx * nc + col

    def plane(d):
        return lax.rem(mx + d // ny, nx), lax.rem(my + d % ny, ny)

    def plane_from(d):
        return lax.rem(mx + nx - d // ny, nx), lax.rem(my + ny - d % ny, ny)

    def side(d):
        return lax.rem(mx + d // nc, nx), lax.rem(col + d % nc, nc)

    def side_from(d):
        return lax.rem(mx + nx - d // nc, nx), lax.rem(col + nc - d % nc, nc)

    core_copy = pltpu.make_async_copy(core_hbm, core_v, core_sem)
    core_copy.start()

    barrier = pltpu.get_barrier_semaphore()

    def signal_plane(d, _):
        a, b = plane(d)
        pl.semaphore_signal(barrier, inc=1, device_id=(a, b, col), device_id_type=MESH)
        return 0

    def signal_side(d, _):
        a, c = side(d)
        pl.semaphore_signal(barrier, inc=1, device_id=(a, my, c), device_id_type=MESH)
        return 0

    lax.fori_loop(1, n_s, signal_plane, 0)
    lax.fori_loop(1, nx * nc, signal_side, 0)

    h, l = halves(ktu_ref[...])
    ktu_s[0], ktu_s[1] = h, l
    h, l = halves(kf1_ref[...])
    kf1_s[0], kf1_s[1] = h, l

    kin = halves(kin_ref[...])
    for b in range(b_loc):
        right = jnp.concatenate(
            [spec_ref[c, b].reshape(cin * kx_loc, lanes) for c in range(2)], axis=1
        )
        got = dot_split(kin, halves(right))
        for c in range(2):
            piece = got[:, c * lanes : (c + 1) * lanes]
            xs[:, c, b] = piece.reshape(nc, p_loc, kx_loc, lanes)

    pl.semaphore_wait(barrier, n_s - 1 + nx * nc - 1)

    def x_copy(d):
        a, c = side(d)
        return pltpu.make_async_remote_copy(
            src_ref=xs.at[c], dst_ref=X.at[mx, col],
            send_sem=xsend.at[d], recv_sem=xrecv.at[d],
            device_id=(a, my, c), device_id_type=MESH,
        )

    def x_arrival(d):
        a, c = side_from(d)
        return pltpu.make_async_remote_copy(
            src_ref=xs.at[c], dst_ref=X.at[a, c],
            send_sem=xsend.at[d], recv_sem=xrecv.at[d],
            device_id=(a, my, c), device_id_type=MESH,
        )

    def e_copy(k, d):
        a, b = plane(d)
        return pltpu.make_async_remote_copy(
            src_ref=E.at[k, a * ny + b], dst_ref=G.at[k, me_s],
            send_sem=esend.at[k, d], recv_sem=erecv.at[k, d],
            device_id=(a, b, col), device_id_type=MESH,
        )

    def e_arrival(k, d):
        a, b = plane_from(d)
        return pltpu.make_async_remote_copy(
            src_ref=E.at[k, me_s], dst_ref=G.at[k, a * ny + b],
            send_sem=esend.at[k, d], recv_sem=erecv.at[k, d],
            device_id=(a, b, col), device_id_type=MESH,
        )

    def y_copy(d):
        a, c = side(d)
        return pltpu.make_async_remote_copy(
            src_ref=Y.at[a, c], dst_ref=R.at[mx, col],
            send_sem=ysend.at[d], recv_sem=yrecv.at[d],
            device_id=(a, my, c), device_id_type=MESH,
        )

    def y_arrival(d):
        a, c = side_from(d)
        return pltpu.make_async_remote_copy(
            src_ref=Y.at[mx, col], dst_ref=R.at[a, c],
            send_sem=ysend.at[d], recv_sem=yrecv.at[d],
            device_id=(a, my, c), device_id_type=MESH,
        )

    def each(low, high, act):
        def step(d, _):
            act(d)
            return 0

        lax.fori_loop(low, high, step, 0)

    each(1, nx * nc, lambda d: x_copy(d).start())
    X[mx, col] = xs[col]
    core_copy.wait()

    for k in range(chunks):
        for c in range(2):
            def expand(g, _):
                base = g * group
                left = jnp.concatenate(
                    [core_v[c, k * pc + base + i].T for i in range(group)], axis=0
                )
                got = dot_split(halves(left), (ktu_s[0], ktu_s[1]))
                for i in range(group):
                    for a in range(nx):
                        row = i * q_all + a * q_loc
                        for b in range(ny):
                            E[k, a * ny + b, c, base + i] = got[
                                row : row + q_loc, b * lanes : (b + 1) * lanes
                            ]
                return 0

            lax.fori_loop(0, pc // group, expand, 0)
        each(1, n_s, lambda d: e_copy(k, d).start())
        G[k, me_s] = E[k, me_s]

    each(1, nx * nc, lambda d: x_arrival(d).wait_recv())

    for k in range(chunks):
        each(1, n_s, lambda d: e_arrival(k, d).wait_recv())

        for g in range(pc // group):
            first = k == 0 and g == 0

            def weigh(i, _):
                right = jnp.concatenate(
                    [
                        G[k, :, c, g * group + i].reshape(n_s * q_loc, lanes)
                        for c in range(2)
                    ],
                    axis=1,
                )
                got = dot_split((kf1_s[0], kf1_s[1]), halves(right))
                got = got.reshape(nx, q_loc, kx_loc, 2 * lanes)
                W[i, :, 0] = got[..., :lanes]
                W[i, :, 1] = got[..., lanes:]
                return 0

            lax.fori_loop(0, group, weigh, 0)

            def add_up(j, _):
                a, rest = j // (nc * b_loc), j % (nc * b_loc)
                s, b = rest // b_loc, rest % b_loc
                real = imag = None
                for i in range(group):
                    p = k * pc + g * group + i
                    xr, xi = X[a, s, 0, b, p], X[a, s, 1, b, p]
                    wr, wi = W[i, a, 0], W[i, a, 1]
                    re = xr * wr - xi * wi
                    im = xr * wi + xi * wr
                    real = re if real is None else real + re
                    imag = im if imag is None else imag + im
                if first:
                    Y[a, s, 0, b] = real
                    Y[a, s, 1, b] = imag
                else:
                    Y[a, s, 0, b] += real
                    Y[a, s, 1, b] += imag
                return 0

            lax.fori_loop(0, nx * nc * b_loc, add_up, 0)

    each(1, nx * nc, lambda d: y_copy(d).start())
    R[mx, col] = Y[mx, col]
    kout = halves(kout_ref[...])
    each(1, nx * nc, lambda d: x_copy(d).wait_send())
    for k in range(chunks):
        each(1, n_s, lambda d: e_copy(k, d).wait_send())
    each(1, nx * nc, lambda d: y_arrival(d).wait_recv())

    for b in range(b_loc):
        columns = []
        for c in range(2):
            total = R[:, 0, c, b]
            for s in range(1, nc):
                total = total + R[:, s, c, b]
            columns.append(total.reshape(q_all * kx_loc, lanes))
        got = dot_split(kout, halves(jnp.concatenate(columns, axis=1)))
        for c in range(2):
            out_ref[c, b] = got[:, c * lanes : (c + 1) * lanes].reshape(
                cout, kx_loc, lanes
            )
    each(1, nx * nc, lambda d: y_copy(d).wait_send())


def per_device(
    nx, ny, nc,
    spectrum, core_tensor, input_factor, output_factor, first_factor, second_factor, third_factor,
):
    _, b_loc, cin, kx_loc, lanes = spectrum.shape
    _, p_loc, q_all, _, r4, r5 = core_tensor.shape
    cout = output_factor.shape[0]
    n_s = nx * ny
    q_loc = q_all // nx
    chunks = 4
    pc = p_loc // chunks
    group = 4 if pc % 4 == 0 else pc

    both = jnp.concatenate([first_factor, second_factor], axis=0)
    both = lax.all_gather(both, ("mx", "my"), axis=0)
    both = both.reshape(nx, ny, both.shape[1], both.shape[2])
    first = both[:, 0, :kx_loc]
    second = both[0, :, kx_loc:].reshape(-1, r4)

    core = jnp.transpose(core_tensor, (0, 1, 3, 4, 5, 2)).reshape(2, p_loc, r4 * r5, q_all)
    eye = jnp.eye(kx_loc, dtype=F32)
    kin = (input_factor.T[:, None, :, None] * eye[None, :, None, :]).reshape(
        -1, cin * kx_loc
    )
    kout = (output_factor[:, None, :, None] * eye[None, :, None, :]).reshape(
        cout * kx_loc, -1
    )
    ktu = (second.T[:, None, :, None] * third_factor.T[None, :, None, :]).reshape(r4 * r5, -1)
    eye_q = jnp.eye(q_loc, dtype=F32)
    kf1 = (first[:, None, :, :, None] * eye_q[None, :, None, None, :]).reshape(
        nx * q_loc * kx_loc, n_s * q_loc
    )
    vmem = pl.BlockSpec(memory_space=pltpu.VMEM)
    return pl.pallas_call(
        functools.partial(kernel, (nx, ny, nc, chunks, pc, group)),
        out_shape=jax.ShapeDtypeStruct((2, b_loc, cout, kx_loc, lanes), F32),
        in_specs=[vmem, pl.BlockSpec(memory_space=pl.ANY), vmem, vmem, vmem, vmem],
        out_specs=vmem,
        scratch_shapes=[
            pltpu.VMEM(core.shape, F32),
            pltpu.VMEM((nc, 2, b_loc, p_loc, kx_loc, lanes), F32),
            pltpu.VMEM((nx, nc, 2, b_loc, p_loc, kx_loc, lanes), F32),
            pltpu.VMEM((chunks, n_s, 2, pc, q_loc, lanes), F32),
            pltpu.VMEM((chunks, n_s, 2, pc, q_loc, lanes), F32),
            pltpu.VMEM((nx, nc, 2, b_loc, q_loc, kx_loc, lanes), F32),
            pltpu.VMEM((nx, nc, 2, b_loc, q_loc, kx_loc, lanes), F32),
            pltpu.VMEM((group, nx, 2, q_loc, kx_loc, lanes), F32),
            pltpu.VMEM((2,) + ktu.shape, BF16),
            pltpu.VMEM((2,) + kf1.shape, BF16),
            pltpu.SemaphoreType.DMA,
            pltpu.SemaphoreType.DMA((nx * nc,)),
            pltpu.SemaphoreType.DMA((nx * nc,)),
            pltpu.SemaphoreType.DMA((chunks, n_s)),
            pltpu.SemaphoreType.DMA((chunks, n_s)),
            pltpu.SemaphoreType.DMA((nx * nc,)),
            pltpu.SemaphoreType.DMA((nx * nc,)),
        ],
        compiler_params=pltpu.CompilerParams(
            collective_id=0, has_side_effects=True, vmem_limit_bytes=60000 * 1024
        ),
    )(spectrum, core, kin, ktu, kf1, kout)


def solution(mesh):
    placed = (
        P(None, "col", None, "mx", "my"),
        P(None, "col", None, ("mx", "my"), None, None),
        P(),
        P(),
        P("mx", None),
        P("my", None),
        P(),
    )
    return jax.shard_map(
        functools.partial(
            per_device, mesh.shape["mx"], mesh.shape["my"], mesh.shape["col"]
        ),
        mesh=mesh,
        in_specs=placed,
        out_specs=P(None, "col", None, "mx", "my"),
        check_vma=False,
    )
```
